32 devices in a mesh: seq: 4 (over y, x), grp: 8 (over z, core).
Axes of the slice: x: 2, y: 2, z: 4, core: 2. Of those that a mesh axis runs over, the one named last changes fastest.
Arguments:
- conv_input: bfloat16 [8, 2048, 5120], P('grp', 'seq'), may hold values from -6 to 6
- step_raw: float32 [8, 64, 2048], P('grp', None, 'seq'), may hold values from -5 to 0
- decay_rate: float32 [64], replicated, may hold values from 0 to 2, as said below
- conv_weight: bfloat16 [4, 5120], replicated, may hold values from -3 to 3
- conv_bias: bfloat16 [5120], replicated, may hold values from -3 to 3
- norm_gain: float32 [4096], replicated, may hold values from 0.5 to 1.5
- owner_slot: int32 [8], replicated, may hold values from 0 to 7, each once
Outputs:
- mixed: bfloat16 [8, 2048, 4096], P('grp', 'seq')
- final_ssm: float32 [8, 64, 64, 128], P('seq', 'grp')
- final_conv: bfloat16 [8, 5120, 4], P('seq', 'grp')
The draws below stay inside these ranges and needn't reach their ends.
Inputs may be any that keep to these rules, and one draw needn't show every extreme that they name: `decay_rate`: positive. `owner_slot`: every decode row receives exactly one prompt.
All inputs are finite; a program needn't handle non-finite values.
Results may differ from the reference program's by a relative error of at most 0.009.
Values may be sent and summed in bfloat16 or wider, within the bound.
A program may use at most 128 MiB of HBM per device.

```python
import math
import jax
import jax.numpy as jnp
from jax import lax

HEADS = 64
HEAD_DIM = 64
STATE = 128
GROUPS = 4
CONV_K = 4
BLOCK = 256
L_DEV = 512
D_IN = 4096
CH = 5120
LENGTH = 2048
PROMPTS = 8


def draw_step_raw(key, part):
    noise_key = jax.random.fold_in(key, 11)
    offset_key = jax.random.fold_in(key, 12)
    segments = LENGTH // L_DEV
    noise = 0.5 * jax.random.truncated_normal(noise_key, -3.0, 3.0, (PROMPTS, HEADS, LENGTH), jnp.float32)
    offset = jax.random.uniform(offset_key, (PROMPTS, 1, segments, 1), jnp.float32, -3.5, -2.0)
    offset = jnp.broadcast_to(offset, (PROMPTS, 1, segments, L_DEV)).reshape(PROMPTS, 1, LENGTH)
    return noise + offset


def draw_decay_rate(key, part):
    pick_key = jax.random.fold_in(key, 21)
    fast_key = jax.random.fold_in(key, 22)
    slow_key = jax.random.fold_in(key, 23)
    share = 0.5
    quick = jax.random.uniform(pick_key, (HEADS,), jnp.float32) < share
    fast_rate = jnp.exp(jax.random.uniform(fast_key, (HEADS,), jnp.float32, math.log(0.5), math.log(2.0)))
    slow_rate = jnp.exp(jax.random.uniform(slow_key, (HEADS,), jnp.float32, math.log(2.0 / LENGTH), math.log(15.0 / LENGTH)))
    return jnp.where(quick, fast_rate, slow_rate)


def block_levels(own_key, dims, shards, least, high):
    level, own = 1.0, jax.random.fold_in(own_key, 6)
    for position, blocks in shards:
        heights = jnp.exp(jax.random.uniform(jax.random.fold_in(own, position), (blocks,), jnp.float32, least / len(shards), high / len(shards)))
        level = level * jnp.repeat(heights, dims[position] // blocks).reshape([-1 if axis == position else 1 for axis in range(len(dims))])
    return level


def scatter_about(own_key, shape, scale, limit, cuts=(), kind=jnp.bfloat16):
    drawn = scale * jax.random.normal(own_key, shape, jnp.float32)
    if cuts:
        drawn = drawn * block_levels(own_key, shape, cuts, -0.22, 0.18)
    return jnp.clip(drawn, -limit, limit).astype(kind)


def setup_inputs(seed: int = 0) -> dict:
    streams_of = jax.random.split(jax.random.key(seed), 8)
    conv_input = scatter_about(streams_of[0], (PROMPTS, LENGTH, CH), 1.0, 6.0, ((0, 8), (1, 4)))
    step_raw = draw_step_raw(jax.random.fold_in(streams_of[7], 71), 0)
    decay_rate = draw_decay_rate(jax.random.fold_in(streams_of[7], 71), 0)
    conv_weight = scatter_about(streams_of[3], (CONV_K, CH), CONV_K ** -0.5, 3.0)
    conv_bias = scatter_about(streams_of[4], (CH,), 0.5, 3.0)
    norm_gain = jnp.clip(1.0 + 0.1 * jax.random.normal(streams_of[5], (D_IN,), jnp.float32), 0.5, 1.5)
    owner_slot = jax.random.permutation(streams_of[6], PROMPTS).astype(jnp.int32)
    return dict(conv_input=conv_input, step_raw=step_raw, decay_rate=decay_rate, conv_weight=conv_weight, conv_bias=conv_bias, norm_gain=norm_gain, owner_slot=owner_slot)


NORM_EPS = 1.0

def conv_silu(padded, conv_weight, conv_bias):
    width = conv_weight.shape[0]
    length = padded.shape[0] - width + 1
    total = jnp.zeros((length, padded.shape[1]), jnp.float32) + conv_bias.astype(jnp.float32)[None, :]
    for offset in range(width):
        total = total + conv_weight[offset].astype(jnp.float32)[None, :] * padded[offset:offset + length].astype(jnp.float32)
    return jax.nn.silu(total).astype(jnp.bfloat16)

def rounded(value):
    return lax.optimization_barrier(value.astype(jnp.bfloat16)).astype(jnp.float32)

def block_terms(inputs, b_matrix, c_matrix, step_size, log_decay):
    width = log_decay.shape[-1]
    summed = jnp.cumsum(log_decay, axis=-1)
    scores = jnp.einsum('tgn,ugn->gtu', c_matrix.astype(jnp.float32), b_matrix.astype(jnp.float32))
    causal = jnp.arange(width)[:, None] >= jnp.arange(width)[None, :]
    spread = jnp.exp(jnp.minimum(summed[:, :, :, None] - summed[:, :, None, :], 0.0))
    weights = jnp.where(causal, spread, 0.0) * step_size[:, :, None, :] * scores[:, None, :, :]
    intra = jnp.einsum('gktu,ugkp->tgkp', rounded(weights), inputs.astype(jnp.float32))
    tail = jnp.exp(summed[:, :, -1:] - summed) * step_size
    scaled = tail[..., None] * jnp.swapaxes(b_matrix, 0, 1).astype(jnp.float32)[:, None, :, :]
    local = jnp.einsum('gkun,ugkp->gkpn', rounded(scaled), inputs.astype(jnp.float32))
    return (intra, local, jnp.exp(summed[:, :, -1]), jnp.exp(summed))

def from_state(c_matrix, carried, scale):
    reach = jnp.einsum('tgn,gkpn->tgkp', c_matrix.astype(jnp.float32), rounded(carried))
    return reach * jnp.transpose(scale, (2, 0, 1))[..., None]

def one_prompt(conv_rows, raw_steps, decay_rate, conv_weight, conv_bias, norm_gain):
    width = conv_weight.shape[0]
    padded = jnp.concatenate([jnp.zeros((width - 1, conv_rows.shape[1]), conv_rows.dtype), conv_rows], axis=0)
    conved = conv_silu(padded, conv_weight, conv_bias)
    blocks = LENGTH // BLOCK
    per_group = HEADS // GROUPS
    inputs = conved[:, :D_IN].reshape(blocks, BLOCK, GROUPS, per_group, HEAD_DIM)
    b_matrix = conved[:, D_IN:D_IN + GROUPS * STATE].reshape(blocks, BLOCK, GROUPS, STATE)
    c_matrix = conved[:, D_IN + GROUPS * STATE:].reshape(blocks, BLOCK, GROUPS, STATE)
    step_size = jax.nn.softplus(raw_steps)
    log_decay = -step_size * decay_rate[:, None]
    step_size = jnp.moveaxis(step_size.reshape(GROUPS, per_group, blocks, BLOCK), 2, 0)
    log_decay = jnp.moveaxis(log_decay.reshape(GROUPS, per_group, blocks, BLOCK), 2, 0)

    def advance(carried, pieces):
        intra, local, decay, scale = block_terms(pieces[0], pieces[1], pieces[2], pieces[3], pieces[4])
        output = intra + from_state(pieces[2], carried, scale)
        return (decay[:, :, None, None] * carried + local, output)
    start = jnp.zeros((GROUPS, per_group, HEAD_DIM, STATE), jnp.float32)
    final, outputs = lax.scan(advance, start, (inputs, b_matrix, c_matrix, step_size, log_decay))
    values = outputs.reshape(LENGTH, GROUPS, per_group * HEAD_DIM)
    norm_scale = lax.rsqrt(lax.optimization_barrier(jnp.mean(values * values, axis=-1)) + NORM_EPS)
    mixed = ((values * norm_scale[..., None]).reshape(LENGTH, D_IN) * norm_gain[None, :]).astype(jnp.bfloat16)
    kept = jnp.transpose(conv_rows[LENGTH - width:], (1, 0))
    return (mixed, final.reshape(HEADS, HEAD_DIM, STATE), kept)

def reference(conv_input, step_raw, decay_rate, conv_weight, conv_bias, norm_gain, owner_slot):

    def run(pieces):
        return one_prompt(pieces[0], pieces[1], decay_rate, conv_weight, conv_bias, norm_gain)
    mixed, final_state, kept = lax.map(run, (conv_input, step_raw))
    final_ssm = jnp.zeros_like(final_state).at[owner_slot].set(final_state)
    final_conv = jnp.zeros_like(kept).at[owner_slot].set(kept)
    return (mixed, final_ssm, final_conv)
```

```python
import functools
import math

import jax
import jax.numpy as jnp
from jax import lax
from jax.experimental import pallas as pl
from jax.experimental.pallas import tpu as pltpu
from jax.sharding import PartitionSpec as P

HEAD_DIM = 64
STATE = 128
GROUPS = 4
SUB = 128
HALO = 8
NORM_EPS = 1.0
LOG2E = math.log2(math.e)
F32 = jnp.float32
BF16 = jnp.bfloat16
NEG = -1e30


def split_rows(value):
    high = value.astype(BF16).astype(F32)
    return jnp.concatenate([high, value - high], axis=0).T.astype(BF16)


def step_kernel(raw_ref, rate_ref, col_ref, row_ref, tail_ref, near_ref, full_ref, log_ref):
    heads, length = raw_ref.shape
    per = heads // GROUPS
    u = lax.broadcasted_iota(jnp.int32, (SUB, SUB), 0)
    t = lax.broadcasted_iota(jnp.int32, (SUB, SUB), 1)
    upper = jnp.where(u <= t, 1.0, 0.0).astype(F32)
    base = jnp.zeros((heads, 1), F32)
    for j in range(length // SUB):
        cut = slice(j * SUB, (j + 1) * SUB)
        raw = raw_ref[:, cut]
        dt = jnp.maximum(raw, 0.0) + jnp.log(1.0 + jnp.exp(-jnp.abs(raw)))
        rate = dt * (rate_ref[...] * -LOG2E)
        cs = jnp.dot(rate, upper, precision=lax.Precision.HIGHEST, preferred_element_type=F32)
        q = cs - jnp.log(dt) * LOG2E
        row_ref[:, cut] = q
        total = cs[:, SUB - 1 :]
        turned = cs.T
        for g in range(GROUPS):
            col_ref[g, cut, :] = turned[:, g * per : (g + 1) * per]
        tail_ref[cut, :] = split_rows(jnp.exp2(total - q))
        near_ref[cut, :] = split_rows(jnp.exp2(cs))
        full_ref[cut, :] = split_rows(jnp.exp2(cs + base))
        base = base + total
    log_ref[...] = base


def conv_silu(buf, w_ref, b_ref, cols):
    total = b_ref[:, cols].astype(F32)
    width = w_ref.shape[0]
    for k in range(width):
        start = HALO - width + 1 + k
        total = total + w_ref[k : k + 1, cols].astype(F32) * buf[start : start + SUB, cols]
    half = 0.5 * total
    return half + half * jnp.tanh(half)


def state_kernel(
    x_ref, b_ref, c_ref, hx_ref, hb_ref, hc_ref, wx_ref, wb_ref, wc_ref, bx_ref, bb_ref, bc_ref,
    tail_ref, near_ref, exp_ref, xo_ref, bo_ref, co_ref, prev_ref, end_ref, endt_ref,
    state, xbuf, bbuf, cbuf,
):
    j = pl.program_id(1)
    last = pl.num_programs(1) - 1
    trios = ((xbuf, x_ref, hx_ref), (bbuf, b_ref, hb_ref), (cbuf, c_ref, hc_ref))

    @pl.when(j == 0)
    def _():
        state[...] = jnp.zeros_like(state)
        for buf, _, h_ref in trios:
            buf[:HALO, :] = h_ref[...].astype(F32)

    @pl.when(j > 0)
    def _():
        for buf, _, _ in trios:
            buf[:HALO, :] = buf[SUB:, :]

    for buf, ref, _ in trios:
        buf[HALO:, :] = ref[...].astype(F32)
    whole = slice(0, STATE)
    b = conv_silu(bbuf, wb_ref, bb_ref, whole).astype(BF16)
    bo_ref[...] = b
    co_ref[...] = conv_silu(cbuf, wc_ref, bc_ref, whole).astype(BF16)
    wide = x_ref.shape[1]
    for n in range(wide // 256):
        cols = slice(n * 256, (n + 1) * 256)
        tail = jnp.dot(tail_ref[...], exp_ref[:, cols], preferred_element_type=F32)
        decay = jnp.dot(near_ref[SUB - 8 :, :], exp_ref[:, cols], preferred_element_type=F32)[7:8, :]
        x = conv_silu(xbuf, wx_ref, bx_ref, cols).astype(BF16)
        xo_ref[:, cols] = x
        scaled = (x.astype(F32) * tail).astype(BF16)
        local = lax.dot_general(b, scaled, (((0,), (0,)), ((), ())), preferred_element_type=F32)
        old = state[:, cols]
        prev_ref[0, :, cols] = old.astype(BF16)
        state[:, cols] = decay * old + local

    @pl.when(j == last)
    def _():
        end_ref[...] = state[...].astype(BF16)
        for n in range(wide // 128):
            cols = slice(n * 128, (n + 1) * 128)
            endt_ref[cols, :] = state[:, cols].T


def intra_kernel(x_ref, b_ref, c_ref, prev_ref, col_ref, row_ref, near_ref, exp_ref, y_ref):
    b, c = b_ref[...], c_ref[...]
    scores = lax.dot_general(c, b, (((1,), (1,)), ((), ())), preferred_element_type=F32)
    t = lax.broadcasted_iota(jnp.int32, (SUB, SUB), 0)
    u = lax.broadcasted_iota(jnp.int32, (SUB, SUB), 1)
    causal = u <= t
    low = lax.broadcasted_iota(jnp.int32, (SUB, 2 * HEAD_DIM), 1) < HEAD_DIM
    zero = jnp.zeros((SUB, 2 * HEAD_DIM), BF16)
    wide = x_ref.shape[1]
    for n in range(wide // (2 * HEAD_DIM)):
        cols = slice(n * 128, (n + 1) * 128)
        parts = []
        for k in (2 * n, 2 * n + 1):
            gap = col_ref[0, :, k : k + 1] - row_ref[k : k + 1, :]
            parts.append((jnp.exp2(jnp.where(causal, gap, NEG)) * scores).astype(BF16))
        x = x_ref[:, cols]
        pair = jnp.concatenate([jnp.where(low, x, zero), jnp.where(low, zero, x)], axis=0)
        weights = jnp.concatenate(parts, axis=1)
        y = jnp.dot(weights, pair, preferred_element_type=F32)
        reach = jnp.dot(c, prev_ref[0, :, cols], preferred_element_type=F32)
        near = jnp.dot(near_ref[...], exp_ref[:, cols], preferred_element_type=F32)
        y_ref[:, cols] = y + near * reach


def norm_kernel(hops, y_ref, c_ref, full_ref, exp_ref, coef_ref, gain_ref, *rest):
    got, out_ref, state, buf = rest[:hops], rest[hops], rest[hops + 1], rest[hops + 2]

    @pl.when(pl.program_id(1) == 0)
    def _():
        total = coef_ref[0:1, :] * got[0][...].astype(F32)
        for k in range(1, hops):
            total = total + coef_ref[k : k + 1, :] * got[k][...].astype(F32)
        state[...] = total.astype(BF16)

    wide = y_ref.shape[1]
    squares = jnp.zeros((SUB, 128), F32)
    for n in range(wide // 256):
        cols = slice(n * 256, (n + 1) * 256)
        reach = jnp.dot(c_ref[...], state[:, cols], preferred_element_type=F32)
        scale = jnp.dot(full_ref[...], exp_ref[:, cols], preferred_element_type=F32)
        y = y_ref[:, cols] + scale * reach
        buf[:, cols] = y
        y2 = y * y
        squares = squares + y2[:, :128] + y2[:, 128:]
    norm = lax.rsqrt(jnp.sum(squares, axis=1, keepdims=True) * (1.0 / wide) + NORM_EPS)
    for n in range(wide // 256):
        cols = slice(n * 256, (n + 1) * 256)
        out_ref[:, cols] = (buf[:, cols] * norm * gain_ref[:, cols]).astype(BF16)


def place_kernel(slot_ref, got_ref, out_ref):
    out_ref[...] = got_ref[...]


def cost(flops, nbytes):
    return pl.CostEstimate(flops=flops, bytes_accessed=nbytes, transcendentals=0)


def body(conv_input, step_raw, decay_rate, conv_weight, conv_bias, norm_gain, owner_slot):
    seq, ngrp = lax.axis_size("seq"), lax.axis_size("grp")
    place = lax.axis_index("seq")
    width = conv_weight.shape[0]
    rows = conv_input[0]
    length, chans = rows.shape
    heads = step_raw.shape[1]
    per = heads // GROUPS
    d_in = heads * HEAD_DIM
    wide = d_in // GROUPS
    blocks = length // SUB
    slots = owner_slot.shape[0]
    shape = jax.ShapeDtypeStruct

    def along(value, distance):
        return lax.ppermute(value, "seq", [(i, i + distance) for i in range(seq - distance)])

    halo = along(rows[length - HALO :], 1)
    cols_t, rows_q, tail, near, full, shard_log = pl.pallas_call(
        step_kernel,
        out_shape=(
            shape((GROUPS, length, per), F32),
            shape((heads, length), F32),
            shape((length, 2 * heads), BF16),
            shape((length, 2 * heads), BF16),
            shape((length, 2 * heads), BF16),
            shape((heads, 1), F32),
        ),
        cost_estimate=cost(10**7, 10**6),
    )(step_raw[0], decay_rate[:, None])
    shard_log = shard_log[:, 0]
    logs = lax.all_gather(shard_log, "seq", axis=0)

    picks = jnp.arange(2 * heads)[:, None] % heads == jnp.arange(d_in)[None, :] // HEAD_DIM
    expand = picks.astype(BF16)
    bias = conv_bias[None, :]
    b_at, c_at = d_in // STATE, d_in // STATE + GROUPS

    def x_spec(height, moves=False):
        return pl.BlockSpec((height, wide), lambda g, j: (j if moves else 0, g))

    def bc_spec(height, at, moves=False):
        return pl.BlockSpec((height, STATE), lambda g, j: (j if moves else 0, at + g))

    tall = pl.BlockSpec((SUB, 2 * heads), lambda g, j: (j, 0))
    exp_spec = pl.BlockSpec((2 * heads, wide), lambda g, j: (0, g))
    prev_spec = pl.BlockSpec((1, STATE, wide), lambda g, j: (j, 0, g))
    trio = lambda h, m: [x_spec(h, m), bc_spec(h, b_at, m), bc_spec(h, c_at, m)]
    xc, bc, cc, prev, end, end_t = pl.pallas_call(
        state_kernel,
        grid=(GROUPS, blocks),
        in_specs=trio(SUB, True) + trio(HALO, False) + trio(width, False) + trio(1, False)
        + [tall, tall, exp_spec],
        out_specs=[
            x_spec(SUB, True), bc_spec(SUB, 0, True), bc_spec(SUB, 0, True), prev_spec,
            pl.BlockSpec((STATE, wide), lambda g, j: (0, g)),
            pl.BlockSpec((wide, STATE), lambda g, j: (g, 0)),
        ],
        out_shape=(
            shape((length, d_in), BF16),
            shape((length, GROUPS * STATE), BF16),
            shape((length, GROUPS * STATE), BF16),
            shape((blocks, STATE, d_in), BF16),
            shape((STATE, d_in), BF16),
            shape((d_in, STATE), F32),
        ),
        scratch_shapes=[
            pltpu.VMEM((STATE, wide), F32),
            pltpu.VMEM((HALO + SUB, wide), F32),
            pltpu.VMEM((HALO + SUB, STATE), F32),
            pltpu.VMEM((HALO + SUB, STATE), F32),
        ],
        cost_estimate=cost(10**9, 2 * 10**7),
    )(
        rows, rows, rows, halo, halo, halo, conv_weight, conv_weight, conv_weight,
        bias, bias, bias, tail, near, expand,
    )

    got = [along(end, k) for k in range(1, seq)]

    index = jnp.arange(seq)
    after = (index > place)[:, None]
    later = jnp.exp2(jnp.sum(jnp.where(after, logs, 0.0), axis=0))
    sent_state = (end_t.reshape(heads, HEAD_DIM, STATE) * later[:, None, None]).astype(BF16)
    sent_state = sent_state.reshape(ngrp, -1, STATE)
    kept = rows[length - width :].T.reshape(ngrp, -1, STATE)
    kept = jnp.where(place == seq - 1, kept, jnp.zeros_like(kept))
    sent = jnp.concatenate([sent_state, kept], axis=1)
    swapped = lax.all_to_all(sent, "grp", split_axis=0, concat_axis=0, tiled=True)
    tallness = sent.shape[1]
    placed = pl.pallas_call(
        place_kernel,
        grid_spec=pltpu.PrefetchScalarGridSpec(
            num_scalar_prefetch=1,
            grid=(slots,),
            in_specs=[pl.BlockSpec((1, tallness, STATE), lambda i, slot: (i, 0, 0))],
            out_specs=pl.BlockSpec((1, tallness, STATE), lambda i, slot: (slot[i], 0, 0)),
        ),
        out_shape=shape(swapped.shape, BF16),
        cost_estimate=cost(10**6, 2 * 10**6),
    )(owner_slot, swapped)
    summed = lax.psum_scatter(placed, "seq", scatter_dimension=0, tiled=True)
    mine = sent_state.shape[1]
    final_ssm = summed[:, :mine].astype(F32).reshape(slots // seq, heads // ngrp, HEAD_DIM, STATE)
    final_conv = summed[:, mine:].reshape(slots // seq, chans // ngrp, width)

    y = pl.pallas_call(
        intra_kernel,
        grid=(GROUPS, blocks),
        in_specs=[
            x_spec(SUB, True), bc_spec(SUB, 0, True), bc_spec(SUB, 0, True), prev_spec,
            pl.BlockSpec((1, SUB, per), lambda g, j: (g, j, 0)),
            pl.BlockSpec((per, SUB), lambda g, j: (g, j)),
            tall, exp_spec,
        ],
        out_specs=x_spec(SUB, True),
        out_shape=shape((length, d_in), F32),
        cost_estimate=cost(4 * 10**9, 4 * 10**7),
    )(xc, bc, cc, prev, cols_t, rows_q, near, expand)

    coefs = []
    for k in range(1, seq):
        between = ((index > place - k) & (index < place))[:, None]
        coefs.append(jnp.exp2(jnp.sum(jnp.where(between, logs, 0.0), axis=0)))
    coef = jnp.repeat(jnp.stack(coefs), HEAD_DIM, axis=1)
    hops = seq - 1
    mixed = pl.pallas_call(
        functools.partial(norm_kernel, hops),
        grid=(GROUPS, blocks),
        in_specs=[
            x_spec(SUB, True), bc_spec(SUB, 0, True), tall, exp_spec,
            x_spec(hops), x_spec(1),
        ] + [x_spec(STATE)] * hops,
        out_specs=x_spec(SUB, True),
        out_shape=shape((length, d_in), BF16),
        scratch_shapes=[pltpu.VMEM((STATE, wide), BF16), pltpu.VMEM((SUB, wide), F32)],
        cost_estimate=cost(10**9, 2 * 10**7),
    )(y, cc, full, expand, coef, norm_gain[None, :], *got)
    return (mixed[None], final_ssm, final_conv)


def solution(mesh):
    placed = (P("grp", "seq", None), P("grp", None, "seq"), P(), P(), P(), P(), P())
    return jax.shard_map(
        body,
        mesh=mesh,
        in_specs=placed,
        out_specs=(P("grp", "seq", None), P("seq", "grp", None, None), P("seq", "grp", None)),
        check_vma=False,
    )
```

```python
import functools
import math

import jax
import jax.numpy as jnp
from jax import lax
from jax.experimental import pallas as pl
from jax.experimental.pallas import tpu as pltpu
from jax.sharding import PartitionSpec as P

HEAD_DIM = 64
STATE = 128
GROUPS = 4
SUB = 128
HALO = 8
LOG_ROWS = 16
NORM_EPS = 1.0
LOG2E = math.log2(math.e)
F32 = jnp.float32
BF16 = jnp.bfloat16
NEG = -1e30


def split_rows(value):
    high = value.astype(BF16).astype(F32)
    return jnp.concatenate([high, value - high], axis=0).T.astype(BF16)


def step_kernel(raw_ref, rate_ref, col_ref, row_ref, tail_ref, near_ref, full_ref, log_ref):
    heads, length = raw_ref.shape
    per = heads // GROUPS
    u = lax.broadcasted_iota(jnp.int32, (SUB, SUB), 0)
    t = lax.broadcasted_iota(jnp.int32, (SUB, SUB), 1)
    upper = jnp.where(u <= t, 1.0, 0.0).astype(F32)
    base = jnp.zeros((heads, 1), F32)
    log = jnp.zeros((1, heads), F32)
    for j in range(length // SUB):
        cut = slice(j * SUB, (j + 1) * SUB)
        raw = raw_ref[:, cut]
        dt = jnp.maximum(raw, 0.0) + jnp.log(1.0 + jnp.exp(-jnp.abs(raw)))
        rate = dt * (rate_ref[...] * -LOG2E)
        cs = jnp.dot(rate, upper, precision=lax.Precision.HIGHEST, preferred_element_type=F32)
        q = cs - jnp.log(dt) * LOG2E
        row_ref[:, cut] = q
        total = cs[:, SUB - 1 :]
        turned = cs.T
        for g in range(GROUPS):
            col_ref[g, cut, :] = turned[:, g * per : (g + 1) * per]
        tail_ref[cut, :] = split_rows(jnp.exp2(total - q))
        near_ref[cut, :] = split_rows(jnp.exp2(cs))
        full_ref[cut, :] = split_rows(jnp.exp2(cs + base))
        base = base + total
        log = log + turned[SUB - 1 :, :]
    terms = []
    for _ in range(3):
        high = log.astype(BF16).astype(F32)
        terms.append(high)
        log = log - high
    terms.append(jnp.zeros((LOG_ROWS - 3, heads), F32))
    terms = jnp.concatenate(terms, axis=0)
    log_ref[...] = jnp.concatenate([terms, jnp.zeros_like(terms)], axis=1).astype(BF16)


def conv_silu(buf, w_ref, b_ref, cols, row):
    total = b_ref[:, cols].astype(F32)
    width = w_ref.shape[0]
    for k in range(width):
        start = row + HALO - width + 1 + k
        total = total + w_ref[k : k + 1, cols].astype(F32) * buf[start : start + SUB, cols]
    half = 0.5 * total
    return half + half * jnp.tanh(half)


def state_kernel(
    x_ref, b_ref, c_ref, hx_ref, hb_ref, hc_ref, wx_ref, wb_ref, wc_ref, bx_ref, bb_ref, bc_ref,
    tail_ref, near_ref, log_ref, exp_ref, xo_ref, bo_ref, co_ref, prev_ref, end_ref, endt_ref,
    turned, xbuf, bbuf, cbuf,
):
    length, wide = x_ref.shape
    blocks = length // SUB
    for buf, ref, h_ref in ((bbuf, b_ref, hb_ref), (cbuf, c_ref, hc_ref)):
        buf[:HALO, :] = h_ref[...].astype(F32)
        buf[HALO:, :] = ref[...].astype(F32)
    whole = slice(0, STATE)
    for j in range(blocks):
        cut = slice(j * SUB, (j + 1) * SUB)
        b = conv_silu(bbuf, wb_ref, bb_ref, whole, j * SUB)
        bo_ref[cut, :] = b.astype(BF16)
        turned[j] = b.T.astype(BF16)
        co_ref[cut, :] = conv_silu(cbuf, wc_ref, bc_ref, whole, j * SUB).astype(BF16)

    for n in range(wide // 256):
        cols = slice(n * 256, (n + 1) * 256)
        xbuf[:HALO, :] = hx_ref[:, cols].astype(F32)
        xbuf[HALO:, :] = x_ref[:, cols].astype(F32)
        expand = exp_ref[:, cols]
        state = jnp.zeros((STATE, 256), F32)
        for j in range(blocks):
            cut = slice(j * SUB, (j + 1) * SUB)
            tail = jnp.dot(tail_ref[cut, :], expand, preferred_element_type=F32)
            ends = near_ref[(j + 1) * SUB - 16 : (j + 1) * SUB, :]
            decay = jnp.dot(ends, expand, preferred_element_type=F32)[15:16, :]
            for m in range(2):
                part = slice(n * 256 + m * 128, n * 256 + (m + 1) * 128)
                here = slice(m * 128, (m + 1) * 128)
                total = bx_ref[:, part].astype(F32)
                for k in range(wx_ref.shape[0]):
                    start = j * SUB + HALO - wx_ref.shape[0] + 1 + k
                    total = total + wx_ref[k : k + 1, part].astype(F32) * xbuf[start : start + SUB, here]
                half = 0.5 * total
                xo_ref[cut, part] = (half + half * jnp.tanh(half)).astype(BF16)
            scaled = (xo_ref[cut, cols].astype(F32) * tail).astype(BF16)
            local = jnp.dot(turned[j], scaled, preferred_element_type=F32)
            prev_ref[j, :, cols] = state.astype(BF16)
            state = decay * state + local
        end_ref[:STATE, cols] = state.astype(BF16)
        end_ref[STATE:, cols] = jnp.dot(log_ref[...], expand, preferred_element_type=F32).astype(BF16)
        for m in range(2):
            part = slice(n * 256 + m * 128, n * 256 + (m + 1) * 128)
            endt_ref[part, :] = state[:, m * 128 : (m + 1) * 128].T.astype(BF16)


def intra_kernel(x_ref, b_ref, c_ref, prev_ref, col_ref, row_ref, near_ref, exp_ref, y_ref):
    b, c = b_ref[...], c_ref[...]
    scores = lax.dot_general(c, b, (((1,), (1,)), ((), ())), preferred_element_type=F32)
    t = lax.broadcasted_iota(jnp.int32, (SUB, SUB), 0)
    u = lax.broadcasted_iota(jnp.int32, (SUB, SUB), 1)
    causal = u <= t
    low = lax.broadcasted_iota(jnp.int32, (SUB, 2 * HEAD_DIM), 1) < HEAD_DIM
    zero = jnp.zeros((SUB, 2 * HEAD_DIM), BF16)
    wide = x_ref.shape[1]
    for n in range(wide // (2 * HEAD_DIM)):
        cols = slice(n * 128, (n + 1) * 128)
        parts = []
        for k in (2 * n, 2 * n + 1):
            gap = col_ref[0, :, k : k + 1] - row_ref[k : k + 1, :]
            parts.append((jnp.exp2(jnp.where(causal, gap, NEG)) * scores).astype(BF16))
        x = x_ref[:, cols]
        pair = jnp.concatenate([jnp.where(low, x, zero), jnp.where(low, zero, x)], axis=0)
        weights = jnp.concatenate(parts, axis=1)
        y = jnp.dot(weights, pair, preferred_element_type=F32)
        reach = jnp.dot(c, prev_ref[0, :, cols], preferred_element_type=F32)
        near = jnp.dot(near_ref[...], exp_ref[:, cols], preferred_element_type=F32)
        y_ref[:, cols] = y + near * reach


def norm_kernel(hops, y_ref, c_ref, full_ref, exp_ref, gain_ref, *rest):
    got, out_ref, state, buf, squares = rest[:hops], rest[hops], *rest[hops + 1 :]
    length, wide = y_ref.shape

    def log_of(ref):
        rows = ref[STATE:, :].astype(F32)
        return rows[0:1, :] + rows[1:2, :] + rows[2:3, :]

    total = got[0][:STATE, :].astype(F32)
    since = log_of(got[0])
    for k in range(1, hops):
        total = total + jnp.exp2(since) * got[k][:STATE, :].astype(F32)
        since = since + log_of(got[k])
    state[...] = total.astype(BF16)

    for n in range(wide // 256):
        cols = slice(n * 256, (n + 1) * 256)
        reach = jnp.dot(c_ref[...], state[:, cols], preferred_element_type=F32)
        scale = jnp.dot(full_ref[...], exp_ref[:, cols], preferred_element_type=F32)
        y = y_ref[:, cols] + scale * reach
        buf[:, cols] = y
        y2 = y * y
        more = y2[:, :128] + y2[:, 128:]
        squares[...] = more if n == 0 else squares[...] + more
    for t in range(length // SUB):
        cut = slice(t * SUB, (t + 1) * SUB)
        mean = jnp.sum(squares[cut, :], axis=1, keepdims=True) * (1.0 / wide)
        norm = lax.rsqrt(mean + NORM_EPS)
        for n in range(wide // 128):
            cols = slice(n * 128, (n + 1) * 128)
            out_ref[cut, cols] = (buf[cut, cols] * norm * gain_ref[:, cols]).astype(BF16)


def place_kernel(slot_ref, got_ref, out_ref):
    out_ref[...] = got_ref[...]


def cost(flops, nbytes):
    return pl.CostEstimate(flops=flops, bytes_accessed=nbytes, transcendentals=0)


def body(conv_input, step_raw, decay_rate, conv_weight, conv_bias, norm_gain, owner_slot):
    seq, ngrp = lax.axis_size("seq"), lax.axis_size("grp")
    place = lax.axis_index("seq")
    width = conv_weight.shape[0]
    rows = conv_input[0]
    length, chans = rows.shape
    heads = step_raw.shape[1]
    per = heads // GROUPS
    d_in = heads * HEAD_DIM
    wide = d_in // GROUPS
    blocks = length // SUB
    slots = owner_slot.shape[0]
    shape = jax.ShapeDtypeStruct

    def along(value, distance):
        return lax.ppermute(value, "seq", [(i, i + distance) for i in range(seq - distance)])

    halo = along(rows[length - HALO :], 1)
    cols_t, rows_q, tail, near, full, shard_log = pl.pallas_call(
        step_kernel,
        out_shape=(
            shape((GROUPS, length, per), F32),
            shape((heads, length), F32),
            shape((length, 2 * heads), BF16),
            shape((length, 2 * heads), BF16),
            shape((length, 2 * heads), BF16),
            shape((LOG_ROWS, 2 * heads), BF16),
        ),
        cost_estimate=cost(10**7, 10**6),
    )(step_raw[0], decay_rate[:, None])

    picks = jnp.arange(2 * heads)[:, None] % heads == jnp.arange(d_in)[None, :] // HEAD_DIM
    expand = picks.astype(BF16)
    bias = conv_bias[None, :]
    b_at, c_at = d_in // STATE, d_in // STATE + GROUPS

    def x_spec(height, moves=False):
        return pl.BlockSpec((height, wide), lambda g, j: (j if moves else 0, g))

    def bc_spec(height, at, moves=False):
        return pl.BlockSpec((height, STATE), lambda g, j: (j if moves else 0, at + g))

    tall = pl.BlockSpec((SUB, 2 * heads), lambda g, j: (j, 0))
    exp_spec = pl.BlockSpec((2 * heads, wide), lambda g, j: (0, g))
    prev_spec = pl.BlockSpec((1, STATE, wide), lambda g, j: (j, 0, g))
    strip = lambda height: pl.BlockSpec((height, wide), lambda g: (0, g))
    thin = lambda height, at: pl.BlockSpec((height, STATE), lambda g: (0, at + g))
    flat = lambda height: pl.BlockSpec((height, 2 * heads), lambda g: (0, 0))
    trio = lambda h: [strip(h), thin(h, b_at), thin(h, c_at)]
    xc, bc, cc, prev, end, end_t = pl.pallas_call(
        state_kernel,
        grid=(GROUPS,),
        in_specs=trio(length) + trio(HALO) + trio(width) + trio(1)
        + [flat(length), flat(length), flat(LOG_ROWS), strip(2 * heads)],
        out_specs=[
            strip(length), thin(length, 0), thin(length, 0),
            pl.BlockSpec((blocks, STATE, wide), lambda g: (0, 0, g)),
            strip(STATE + LOG_ROWS),
            pl.BlockSpec((wide, STATE), lambda g: (g, 0)),
        ],
        out_shape=(
            shape((length, d_in), BF16),
            shape((length, GROUPS * STATE), BF16),
            shape((length, GROUPS * STATE), BF16),
            shape((blocks, STATE, d_in), BF16),
            shape((STATE + LOG_ROWS, d_in), BF16),
            shape((d_in, STATE), BF16),
        ),
        scratch_shapes=[
            pltpu.VMEM((blocks, STATE, SUB), BF16),
            pltpu.VMEM((HALO + length, 256), F32),
            pltpu.VMEM((HALO + length, STATE), F32),
            pltpu.VMEM((HALO + length, STATE), F32),
        ],
        cost_estimate=cost(10**9, 2 * 10**7),
    )(
        rows, rows, rows, halo, halo, halo, conv_weight, conv_weight, conv_weight,
        bias, bias, bias, tail, near, shard_log, expand,
    )

    got = [along(end, k) for k in range(1, seq)]

    sent_state = end_t.reshape(ngrp, -1, STATE)
    kept = rows[length - width :].T.reshape(ngrp, -1, STATE)
    log_terms = shard_log[:, :heads].reshape(LOG_ROWS, ngrp, -1).swapaxes(0, 1)
    log_terms = jnp.pad(log_terms, ((0, 0), (0, 0), (0, STATE - log_terms.shape[2])))
    sent = jnp.concatenate([sent_state, kept, log_terms], axis=1)
    swapped = lax.all_to_all(sent, "grp", split_axis=0, concat_axis=0, tiled=True)

    y = pl.pallas_call(
        intra_kernel,
        grid=(GROUPS, blocks),
        in_specs=[
            x_spec(SUB, True), bc_spec(SUB, 0, True), bc_spec(SUB, 0, True), prev_spec,
            pl.BlockSpec((1, SUB, per), lambda g, j: (g, j, 0)),
            pl.BlockSpec((per, SUB), lambda g, j: (g, j)),
            tall, exp_spec,
        ],
        out_specs=x_spec(SUB, True),
        out_shape=shape((length, d_in), F32),
        cost_estimate=cost(4 * 10**9, 4 * 10**7),
    )(xc, bc, cc, prev, cols_t, rows_q, near, expand)

    swapped, y = lax.optimization_barrier((swapped, y))
    tallness = sent.shape[1]
    placed = pl.pallas_call(
        place_kernel,
        grid_spec=pltpu.PrefetchScalarGridSpec(
            num_scalar_prefetch=1,
            grid=(slots,),
            in_specs=[pl.BlockSpec((1, tallness, STATE), lambda i, slot: (i, 0, 0))],
            out_specs=pl.BlockSpec((1, tallness, STATE), lambda i, slot: (slot[i], 0, 0)),
        ),
        out_shape=shape(swapped.shape, BF16),
        cost_estimate=cost(10**6, 2 * 10**6),
    )(owner_slot, swapped)
    owned = lax.all_to_all(placed, "seq", split_axis=0, concat_axis=0, tiled=True)

    hops = seq - 1
    mixed = pl.pallas_call(
        functools.partial(norm_kernel, hops),
        grid=(GROUPS,),
        in_specs=[strip(length), thin(length, 0), flat(length), strip(2 * heads), strip(1)]
        + [strip(STATE + LOG_ROWS)] * hops,
        out_specs=strip(length),
        out_shape=shape((length, d_in), BF16),
        scratch_shapes=[
            pltpu.VMEM((STATE, wide), BF16),
            pltpu.VMEM((length, wide), F32),
            pltpu.VMEM((length, 128), F32),
        ],
        cost_estimate=cost(10**9, 2 * 10**7),
    )(y, cc, full, expand, norm_gain[None, :], *got)

    owned, mixed = lax.optimization_barrier((owned, mixed))
    mine, each = sent_state.shape[1], heads // ngrp
    owned = owned.reshape(seq, slots // seq, tallness, STATE)
    logs = jnp.sum(owned[:, :, -LOG_ROWS : 3 - LOG_ROWS, :each].astype(F32), axis=2)
    index = jnp.arange(seq)
    after = (index[None, :] > index[:, None]).astype(F32)
    weight = jnp.exp2(jnp.sum(after[:, :, None, None] * logs[None], axis=1))
    states = owned[:, :, :mine].reshape(seq, slots // seq, each, HEAD_DIM, STATE)
    final_ssm = jnp.sum(weight[..., None, None] * states.astype(F32), axis=0)
    final_conv = owned[seq - 1, :, mine:-LOG_ROWS].reshape(slots // seq, chans // ngrp, width)
    return (mixed[None], final_ssm, final_conv)


def solution(mesh):
    placed = (P("grp", "seq", None), P("grp", None, "seq"), P(), P(), P(), P(), P())
    return jax.shard_map(
        body,
        mesh=mesh,
        in_specs=placed,
        out_specs=(P("grp", "seq", None), P("seq", "grp", None, None), P("seq", "grp", None)),
        check_vma=False,
    )
```

```python
import functools
import math

import jax
import jax.numpy as jnp
import numpy as np
from jax import lax
from jax.experimental import pallas as pl
from jax.experimental.pallas import tpu as pltpu
from jax.sharding import PartitionSpec as P


HEAD_DIM = 64
STATE = 128
GROUPS = 4
SUB = 128
HALO = 8
LOG_ROWS = 16
NORM_EPS = 1.0
LOG2E = math.log2(math.e)
F32 = jnp.float32
BF16 = jnp.bfloat16
NEG = -1e30


def split_rows(value):
    high = value.astype(BF16).astype(F32)
    return jnp.concatenate([high, value - high], axis=0).T.astype(BF16)


def step_kernel(raw_ref, rate_ref, col_ref, row_ref, tail_ref, near_ref, full_ref, log_ref):
    heads, length = raw_ref.shape
    per = heads // GROUPS
    u = lax.broadcasted_iota(jnp.int32, (SUB, SUB), 0)
    t = lax.broadcasted_iota(jnp.int32, (SUB, SUB), 1)
    upper = jnp.where(u <= t, 1.0, 0.0).astype(F32)
    base = jnp.zeros((heads, 1), F32)
    log = jnp.zeros((1, heads), F32)
    slope = jnp.broadcast_to(rate_ref[...] * -LOG2E, (heads, heads)).T[:, 0:1]
    for j in range(length // SUB):
        cut = slice(j * SUB, (j + 1) * SUB)
        raw = raw_ref[:, cut]
        dt = jnp.maximum(raw, 0.0) + jnp.log(1.0 + jnp.exp(-jnp.abs(raw)))
        rate = dt * slope
        cs = jnp.dot(rate, upper, precision=lax.Precision.HIGHEST, preferred_element_type=F32)
        q = cs - jnp.log(dt) * LOG2E
        row_ref[:, cut] = q
        total = cs[:, SUB - 1 :]
        turned = cs.T
        for g in range(GROUPS):
            col_ref[g, cut, :] = turned[:, g * per : (g + 1) * per]
        tail_ref[cut, :] = split_rows(jnp.exp2(total - q))
        near_ref[cut, :] = split_rows(jnp.exp2(cs))
        full_ref[cut, :] = split_rows(jnp.exp2(cs + base))
        base = base + total
        log = log + turned[SUB - 1 :, :]
    terms = []
    for _ in range(3):
        high = log.astype(BF16).astype(F32)
        terms.append(high)
        log = log - high
    terms.append(jnp.zeros((LOG_ROWS - 3, heads), F32))
    terms = jnp.concatenate(terms, axis=0)
    log_ref[...] = jnp.concatenate([terms, jnp.zeros_like(terms)], axis=1).astype(BF16)


def conv_silu(buf, w_ref, b_ref, cols, row):
    total = b_ref[:, cols].astype(F32)
    width = w_ref.shape[0]
    for k in range(width):
        start = row + HALO - width + 1 + k
        total = total + w_ref[k : k + 1, cols].astype(F32) * buf[start : start + SUB, cols]
    half = 0.5 * total
    return half + half * jnp.tanh(half)


def state_kernel(
    x_ref, b_ref, c_ref, hx_ref, hb_ref, hc_ref, wx_ref, wb_ref, wc_ref, bx_ref, bb_ref, bc_ref,
    tail_ref, near_ref, log_ref, exp_ref, xo_ref, bo_ref, co_ref, prev_ref, end_ref, endt_ref,
    turned, xbuf, bbuf, cbuf,
):
    length, wide = x_ref.shape
    blocks = length // SUB
    for buf, ref, h_ref in ((bbuf, b_ref, hb_ref), (cbuf, c_ref, hc_ref)):
        buf[:HALO, :] = h_ref[...].astype(F32)
        buf[HALO:, :] = ref[...].astype(F32)
    whole = slice(0, STATE)
    for j in range(blocks):
        cut = slice(j * SUB, (j + 1) * SUB)
        b = conv_silu(bbuf, wb_ref, bb_ref, whole, j * SUB)
        bo_ref[cut, :] = b.astype(BF16)
        turned[j] = b.T.astype(BF16)
        co_ref[cut, :] = conv_silu(cbuf, wc_ref, bc_ref, whole, j * SUB).astype(BF16)

    for n in range(wide // 256):
        cols = slice(n * 256, (n + 1) * 256)
        xbuf[:HALO, :] = hx_ref[:, cols].astype(F32)
        xbuf[HALO:, :] = x_ref[:, cols].astype(F32)
        expand = exp_ref[:, cols]
        state = jnp.zeros((STATE, 256), F32)
        for j in range(blocks):
            cut = slice(j * SUB, (j + 1) * SUB)
            tail = jnp.dot(tail_ref[cut, :], expand, preferred_element_type=F32)
            ends = near_ref[(j + 1) * SUB - 16 : (j + 1) * SUB, :]
            decay = jnp.dot(ends, expand, preferred_element_type=F32)[15:16, :]
            for m in range(2):
                part = slice(n * 256 + m * 128, n * 256 + (m + 1) * 128)
                here = slice(m * 128, (m + 1) * 128)
                total = bx_ref[:, part].astype(F32)
                for k in range(wx_ref.shape[0]):
                    start = j * SUB + HALO - wx_ref.shape[0] + 1 + k
                    total = total + wx_ref[k : k + 1, part].astype(F32) * xbuf[start : start + SUB, here]
                half = 0.5 * total
                xo_ref[cut, part] = (half + half * jnp.tanh(half)).astype(BF16)
            scaled = (xo_ref[cut, cols].astype(F32) * tail).astype(BF16)
            local = jnp.dot(turned[j], scaled, preferred_element_type=F32)
            prev_ref[j, :, cols] = state.astype(BF16)
            state = decay * state + local
        end_ref[:STATE, cols] = state.astype(BF16)
        end_ref[STATE:, cols] = jnp.dot(log_ref[...], expand, preferred_element_type=F32).astype(BF16)
        for m in range(2):
            part = slice(n * 256 + m * 128, n * 256 + (m + 1) * 128)
            endt_ref[part, :] = state[:, m * 128 : (m + 1) * 128].T.astype(BF16)


def intra_kernel(x_ref, b_ref, c_ref, prev_ref, col_ref, row_ref, near_ref, exp_ref, y_ref):
    b, c = b_ref[...], c_ref[...]
    scores = lax.dot_general(c, b, (((1,), (1,)), ((), ())), preferred_element_type=F32)
    t = lax.broadcasted_iota(jnp.int32, (SUB, SUB), 0)
    u = lax.broadcasted_iota(jnp.int32, (SUB, SUB), 1)
    causal = u <= t
    low = lax.broadcasted_iota(jnp.int32, (SUB, 2 * HEAD_DIM), 1) < HEAD_DIM
    zero = jnp.zeros((SUB, 2 * HEAD_DIM), BF16)
    wide = x_ref.shape[1]
    for n in range(wide // (2 * HEAD_DIM)):
        cols = slice(n * 128, (n + 1) * 128)
        parts = []
        for k in (2 * n, 2 * n + 1):
            gap = col_ref[0, :, k : k + 1] - row_ref[k : k + 1, :]
            parts.append((jnp.exp2(jnp.where(causal, gap, NEG)) * scores).astype(BF16))
        x = x_ref[:, cols]
        pair = jnp.concatenate([jnp.where(low, x, zero), jnp.where(low, zero, x)], axis=0)
        weights = jnp.concatenate(parts, axis=1)
        y = jnp.dot(weights, pair, preferred_element_type=F32)
        reach = jnp.dot(c, prev_ref[0, :, cols], preferred_element_type=F32)
        near = jnp.dot(near_ref[...], exp_ref[:, cols], preferred_element_type=F32)
        y_ref[:, cols] = y + near * reach


def norm_kernel(hops, y_ref, c_ref, full_ref, exp_ref, gain_ref, *rest):
    got, out_ref, state, buf, squares = rest[:hops], rest[hops], *rest[hops + 1 :]
    length, wide = y_ref.shape

    def log_of(ref):
        rows = ref[STATE:, :].astype(F32)
        return rows[0:1, :] + rows[1:2, :] + rows[2:3, :]

    total = got[0][:STATE, :].astype(F32)
    since = log_of(got[0])
    for k in range(1, hops):
        total = total + jnp.exp2(since) * got[k][:STATE, :].astype(F32)
        since = since + log_of(got[k])
    state[...] = total.astype(BF16)

    for n in range(wide // 256):
        cols = slice(n * 256, (n + 1) * 256)
        reach = jnp.dot(c_ref[...], state[:, cols], preferred_element_type=F32)
        scale = jnp.dot(full_ref[...], exp_ref[:, cols], preferred_element_type=F32)
        y = y_ref[:, cols] + scale * reach
        buf[:, cols] = y
        y2 = y * y
        more = y2[:, :128] + y2[:, 128:]
        squares[...] = more if n == 0 else squares[...] + more
    for t in range(length // SUB):
        cut = slice(t * SUB, (t + 1) * SUB)
        mean = jnp.sum(squares[cut, :], axis=1, keepdims=True) * (1.0 / wide)
        norm = lax.rsqrt(mean + NORM_EPS)
        for n in range(wide // 128):
            cols = slice(n * 128, (n + 1) * 128)
            out_ref[cut, cols] = (buf[cut, cols] * norm * gain_ref[:, cols]).astype(BF16)


def place_kernel(slot_ref, got_ref, out_ref):
    out_ref[...] = got_ref[...]


def cost(flops, nbytes):
    return pl.CostEstimate(flops=flops, bytes_accessed=nbytes, transcendentals=0)


def layer(conv_input, step_raw, decay_rate, conv_weight, conv_bias, norm_gain, owner_slot):
    seq, ngrp = lax.axis_size("seq"), lax.axis_size("grp")
    width = conv_weight.shape[0]
    rows = conv_input[0]
    length, chans = rows.shape
    heads = step_raw.shape[1]
    per = heads // GROUPS
    d_in = heads * HEAD_DIM
    wide = d_in // GROUPS
    blocks = length // SUB
    slots = owner_slot.shape[0]
    shape = jax.ShapeDtypeStruct

    def along(value, distance):
        return lax.ppermute(value, "seq", [(i, i + distance) for i in range(seq - distance)])

    last_rows = rows[length - HALO :]
    halo = along(last_rows, 1)
    cols_t, rows_q, tail, near, full, shard_log = pl.pallas_call(
        step_kernel,
        out_shape=(
            shape((GROUPS, length, per), F32),
            shape((heads, length), F32),
            shape((length, 2 * heads), BF16),
            shape((length, 2 * heads), BF16),
            shape((length, 2 * heads), BF16),
            shape((LOG_ROWS, 2 * heads), BF16),
        ),
        cost_estimate=cost(10**7, 10**6),
    )(step_raw[0], decay_rate[None, :])

    picks = np.arange(2 * heads)[:, None] % heads == np.arange(d_in)[None, :] // HEAD_DIM
    expand = jnp.asarray(picks.astype(BF16))
    bias = conv_bias[None, :]
    b_at, c_at = d_in // STATE, d_in // STATE + GROUPS

    def x_spec(height, moves=False):
        return pl.BlockSpec((height, wide), lambda g, j: (j if moves else 0, g))

    def bc_spec(height, at, moves=False):
        return pl.BlockSpec((height, STATE), lambda g, j: (j if moves else 0, at + g))

    tall = pl.BlockSpec((SUB, 2 * heads), lambda g, j: (j, 0))
    exp_spec = pl.BlockSpec((2 * heads, wide), lambda g, j: (0, g))
    prev_spec = pl.BlockSpec((1, STATE, wide), lambda g, j: (j, 0, g))
    strip = lambda height: pl.BlockSpec((height, wide), lambda g: (0, g))
    thin = lambda height, at: pl.BlockSpec((height, STATE), lambda g: (0, at + g))
    flat = lambda height: pl.BlockSpec((height, 2 * heads), lambda g: (0, 0))
    trio = lambda h: [strip(h), thin(h, b_at), thin(h, c_at)]
    xc, bc, cc, prev, end, end_t = pl.pallas_call(
        state_kernel,
        grid=(GROUPS,),
        in_specs=trio(length) + trio(HALO) + trio(width) + trio(1)
        + [flat(length), flat(length), flat(LOG_ROWS), strip(2 * heads)],
        out_specs=[
            strip(length), thin(length, 0), thin(length, 0),
            pl.BlockSpec((blocks, STATE, wide), lambda g: (0, 0, g)),
            strip(STATE + LOG_ROWS),
            pl.BlockSpec((wide, STATE), lambda g: (g, 0)),
        ],
        out_shape=(
            shape((length, d_in), BF16),
            shape((length, GROUPS * STATE), BF16),
            shape((length, GROUPS * STATE), BF16),
            shape((blocks, STATE, d_in), BF16),
            shape((STATE + LOG_ROWS, d_in), BF16),
            shape((d_in, STATE), BF16),
        ),
        scratch_shapes=[
            pltpu.VMEM((blocks, STATE, SUB), BF16),
            pltpu.VMEM((HALO + length, 256), F32),
            pltpu.VMEM((HALO + length, STATE), F32),
            pltpu.VMEM((HALO + length, STATE), F32),
        ],
        cost_estimate=cost(10**9, 2 * 10**7),
    )(
        rows, rows, rows, halo, halo, halo, conv_weight, conv_weight, conv_weight,
        bias, bias, bias, tail, near, shard_log, expand,
    )

    got = []
    for k in range(1, seq):
        got.append(along(end, k))

    y = pl.pallas_call(
        intra_kernel,
        grid=(GROUPS, blocks),
        in_specs=[
            x_spec(SUB, True), bc_spec(SUB, 0, True), bc_spec(SUB, 0, True), prev_spec,
            pl.BlockSpec((1, SUB, per), lambda g, j: (g, j, 0)),
            pl.BlockSpec((per, SUB), lambda g, j: (g, j)),
            tall, exp_spec,
        ],
        out_specs=x_spec(SUB, True),
        out_shape=shape((length, d_in), F32),
        cost_estimate=cost(4 * 10**9, 4 * 10**7),
    )(xc, bc, cc, prev, cols_t, rows_q, near, expand)


    end_t, last_rows, shard_log, y = lax.optimization_barrier((end_t, last_rows, shard_log, y))
    sent_state = end_t.reshape(ngrp, -1, STATE)
    kept = last_rows[HALO - width :].T.reshape(ngrp, -1, STATE)
    log_terms = shard_log[:, :heads].reshape(LOG_ROWS, ngrp, -1).swapaxes(0, 1)
    log_terms = jnp.pad(log_terms, ((0, 0), (0, 0), (0, STATE - log_terms.shape[2])))
    sent = jnp.concatenate([sent_state, kept, log_terms], axis=1)
    swapped = lax.all_to_all(sent, "grp", split_axis=0, concat_axis=0, tiled=True)
    tallness = sent.shape[1]
    placed = pl.pallas_call(
        place_kernel,
        grid_spec=pltpu.PrefetchScalarGridSpec(
            num_scalar_prefetch=1,
            grid=(slots,),
            in_specs=[pl.BlockSpec((1, tallness, STATE), lambda i, slot: (i, 0, 0))],
            out_specs=pl.BlockSpec((1, tallness, STATE), lambda i, slot: (slot[i], 0, 0)),
        ),
        out_shape=shape(swapped.shape, BF16),
        cost_estimate=cost(10**6, 2 * 10**6),
    )(owner_slot, swapped)
    placed, got = lax.optimization_barrier((placed, got))
    owned = lax.all_to_all(placed, "seq", split_axis=0, concat_axis=0, tiled=True)

    hops = seq - 1
    mixed = pl.pallas_call(
        functools.partial(norm_kernel, hops),
        grid=(GROUPS,),
        in_specs=[strip(length), thin(length, 0), flat(length), strip(2 * heads), strip(1)]
        + [strip(STATE + LOG_ROWS)] * hops,
        out_specs=strip(length),
        out_shape=shape((length, d_in), BF16),
        scratch_shapes=[
            pltpu.VMEM((STATE, wide), BF16),
            pltpu.VMEM((length, wide), F32),
            pltpu.VMEM((length, 128), F32),
        ],
        cost_estimate=cost(10**9, 2 * 10**7),
    )(y, cc, full, expand, norm_gain[None, :], *got)

    owned, mixed = lax.optimization_barrier((owned, mixed))
    mine, each = sent_state.shape[1], heads // ngrp
    owned = owned.reshape(seq, slots // seq, tallness, STATE)
    logs = jnp.sum(owned[:, :, -LOG_ROWS : 3 - LOG_ROWS, :each].astype(F32), axis=2)
    index = jnp.arange(seq)
    after = (index[None, :] > index[:, None]).astype(F32)
    weight = jnp.exp2(jnp.sum(after[:, :, None, None] * logs[None], axis=1))
    states = owned[:, :, :mine].reshape(seq, slots // seq, each, HEAD_DIM, STATE)
    final_ssm = jnp.sum(weight[..., None, None] * states.astype(F32), axis=0)
    final_conv = owned[seq - 1, :, mine:-LOG_ROWS].reshape(slots // seq, chans // ngrp, width)
    return (mixed[None], final_ssm, final_conv)


def solution(mesh):
    placed = (P("grp", "seq", None), P("grp", None, "seq"), P(), P(), P(), P(), P())
    return jax.shard_map(
        layer,
        mesh=mesh,
        in_specs=placed,
        out_specs=(P("grp", "seq", None), P("seq", "grp", None, None), P("seq", "grp", None)),
        check_vma=False,
    )
```
